512 devices in a mesh: dp: 32 (over z_lo, y, core), expert: 16 (over x, z_hi).
Axes of the slice: x: 4, y: 8, z: 8 (z_hi: 4, z_lo: 2; z = z_hi * 2 + z_lo), core: 2. Of those that a mesh axis runs over, the one named last changes fastest.
Arguments:
- grad_out: bfloat16 [4, 32768, 1024], P(None, ('dp', 'expert')), may hold values from -12 to 12
- routes: int32 [4, 32768, 8], P(None, ('dp', 'expert')), may hold values from 0 to 127, all different within a row; in each aligned block of 64 rows (0 to 63, 64 to 127, ..., all dimensions but the last counted through in order) at most 8 rows name the same one
- route_probs: bfloat16 [4, 32768, 8], P(None, ('dp', 'expert')), may hold values from 0.049804688 to 0.3984375
- dispatched: bfloat16 [4, 65536, 1024], P(None, ('dp', 'expert')), may hold values from -12 to 12, as said below
- w_gate: bfloat16 [1024, 4096], P(None, 'expert'), may hold values from -0.1875 to 0.1875
- w_up: bfloat16 [1024, 4096], P(None, 'expert'), may hold values from -0.1875 to 0.1875
- w_down: bfloat16 [4096, 1024], P('expert'), may hold values from -0.25 to 0.25
Outputs:
- grad_in: bfloat16 [4, 32768, 1024], P(None, ('dp', 'expert'))
- grad_gate: float32 [1024, 4096], P('dp', 'expert')
- grad_up: float32 [1024, 4096], P('dp', 'expert')
- grad_down_t: float32 [1024, 4096], P('dp', 'expert')
The draws below stay inside these ranges and needn't reach their ends.
Inputs may be any that keep to these rules, and one draw needn't show every extreme that they name: `routes`: in each micro-batch, among the 64 rows of one device no expert is named more than 8 times, a bound that some expert reaches in some of these blocks. `dispatched`: within each group of 16 consecutive blocks of 128 rows, blocks 2e and 2e + 1 are equal.
All inputs are finite; a program needn't handle non-finite values.
Results may differ from the reference program's by a relative error of at most 0.0058.
Values may be sent and summed in bfloat16 or wider, within the bound.
No kernel may reach another device: no remote copies, remote signals or barrier semaphores. Data moves between devices by JAX's collectives and lax.ppermute only.
A program may use at most 64 MiB of HBM per device.

```python
import math
import jax
import jax.numpy as jnp
import numpy as np
from jax import lax

D = 1024
F = 512
NEXP = 128
TOPK = 8
MB = 4
TOK_DEV = 64
CAPS = 8
EXPERTS = 8
TOKENS = 32768
N_DP = 32
N_EXPERT = 16


def draw_dispatched(key, part):
    shape = (MB, N_DP, N_EXPERT // 2, N_EXPERT * CAPS, D)
    values = jax.random.truncated_normal(key, -4.0, 4.0, shape, jnp.float32)
    doubled = jnp.repeat(values, 2, axis=2)
    return doubled.reshape(MB, N_DP * N_EXPERT * N_EXPERT * CAPS, D).astype(jnp.bfloat16)


def levels(key, shape, shards, smallest, largest):
    gain, own = 1.0, jax.random.fold_in(key, 6)
    for dim, blocks in shards:
        steps = jnp.exp(jax.random.uniform(jax.random.fold_in(own, dim), (blocks,), jnp.float32, smallest / len(shards), largest / len(shards)))
        gain = gain * jnp.repeat(steps, shape[dim] // blocks).reshape([-1 if axis == dim else 1 for axis in range(len(shape))])
    return gain


def shared_out(rng, own, number, rows, number_of, top, limit, skew):
    sequence = jax.random.permutation(rng, number_of)
    heavy_load, ordinary = portions_of(number_of, rows * top, limit, skew, True), portions_of(number_of, rows * top, limit, skew, False)
    places = jnp.arange(number_of)

    def named(lengths, rotation):
        used = int((lengths > 0).sum())
        fixed = max(1, used // 4)
        passed = fixed + (places - fixed + rotation * (used - fixed)) % max(1, number_of - fixed)
        return jnp.zeros((number_of,), jnp.int32).at[sequence[jnp.where(places < fixed, places, passed)]].set(jnp.asarray(lengths, jnp.int32))

    lengths = jnp.where(number % 4 == 0, named(heavy_load, number // 4), named(ordinary, number - number // 4 - 1))
    mixed = jax.random.permutation(jax.random.fold_in(own, 3), number_of)
    source_of, taker = mixed[0:number_of // 2 * 2:2], mixed[1:number_of // 2 * 2:2]
    margin = jnp.minimum(lengths[source_of] - 1, limit - lengths[taker]) // 2
    margin = jnp.where((source_of == sequence[0]) | (taker == sequence[0]) | (lengths[taker] == 0), 0, jnp.maximum(margin, 0))
    passed = jax.random.randint(jax.random.fold_in(own, 4), (number_of // 2,), 0, 1 << 20) % (margin + 1)
    lengths = lengths.at[source_of].add(-passed).at[taker].add(passed)
    items = jnp.searchsorted(jnp.cumsum(lengths), jnp.arange(rows * top), side="right").astype(jnp.int32)
    table = items.reshape(top, rows).T
    table = table[jax.random.permutation(jax.random.fold_in(own, 1), rows)]
    rotation = jax.random.randint(jax.random.fold_in(own, 2), (rows, 1), 0, top)
    return jnp.take_along_axis(table, (jnp.arange(top)[None, :] + rotation) % top, axis=1)


def portions_of(count, total, reach, lean, full):
    loads = [(1 << 20) // math.isqrt(grade ** lean) + 1 for grade in range(1, count + 1)]
    largest = reach if full else min(reach, max(-(-total // count), total * loads[0] // sum(loads)))
    least = 1 if total - largest >= count - 1 else 0
    given, spare = [largest] + [least] * (count - 1), total - largest - least * (count - 1)
    while spare > 0:
        free = [i for i in range(1, count) if given[i] < largest] or [i for i in range(1, count) if given[i] < reach]
        pool, left = sum([loads[i] for i in free]), spare
        for i in free:
            addition = min(reach - given[i], max(1, left * loads[i] // pool), spare)
            given[i] = given[i] + addition
            spare = spare - addition
    return np.array(given)


def scatter_about(own_key, extent, deviation, bound, cuts=(), kind=jnp.bfloat16):
    result = jax.random.normal(own_key, extent, jnp.float32) * deviation
    if len(cuts) > 0:
        result = levels(own_key, extent, cuts, -0.22, 0.18) * result
    return jnp.clip(result, min=-bound, max=bound).astype(kind)


def setup_inputs(seed: int = 0) -> dict:
    splits = jax.random.split(jax.random.key(seed), 8)
    grad_out = scatter_about(splits[0], (MB, TOKENS, D), 3.0, 12.0, ((1, 512),))
    routes_keys = jax.random.split(jax.random.fold_in(splits[1], 1), MB * TOKENS // TOK_DEV)
    routes_turns = jax.random.permutation(jax.random.fold_in(splits[1], 3), MB * TOKENS // TOK_DEV)
    routes = jax.vmap(lambda own, number: shared_out(jax.random.fold_in(splits[1], 2), own, number, TOK_DEV, NEXP, TOPK, CAPS, 1))(routes_keys, routes_turns).reshape((MB, TOKENS, TOPK))
    route_probs = jnp.clip(0.049804688 + 0.3486328 * jax.random.uniform(splits[2], (MB, TOKENS, TOPK), jnp.float32) ** levels(splits[2], (MB, TOKENS, TOPK), ((1, 512),), -0.2, 0.2), 0.049804688, 0.3984375).astype(jnp.bfloat16)
    dispatched = draw_dispatched(jax.random.fold_in(splits[7], 71), 0)
    w_gate = scatter_about(splits[4], (D, EXPERTS * F), D ** -0.5, 0.1875, ((1, 16),))
    w_up = scatter_about(splits[5], (D, EXPERTS * F), D ** -0.5, 0.1875, ((1, 16),))
    w_down = scatter_about(splits[6], (EXPERTS * F, D), F ** -0.5, 0.25, ((0, 16),))
    return {"grad_out": grad_out, "routes": routes, "route_probs": route_probs, "dispatched": dispatched, "w_gate": w_gate, "w_up": w_up, "w_down": w_down}


def expert_backward(rows_in, row_grads, gate_mat, up_mat, down_mat):
    gate_pre = jnp.dot(rows_in, gate_mat, preferred_element_type=jnp.float32)
    up_pre = jnp.dot(rows_in, up_mat, preferred_element_type=jnp.float32)
    sigmoid = jax.nn.sigmoid(gate_pre)
    activated = gate_pre * sigmoid
    hidden = (activated * up_pre).astype(jnp.bfloat16)
    d_down = jnp.dot(row_grads.T, hidden, preferred_element_type=jnp.float32)
    dhidden = jnp.dot(row_grads, down_mat.T, preferred_element_type=jnp.float32)
    d_gate = (dhidden * up_pre * sigmoid * (1.0 + gate_pre * (1.0 - sigmoid))).astype(jnp.bfloat16)
    d_up = (dhidden * activated).astype(jnp.bfloat16)
    grad_gate_e = jnp.dot(rows_in.T, d_gate, preferred_element_type=jnp.float32)
    grad_up_e = jnp.dot(rows_in.T, d_up, preferred_element_type=jnp.float32)
    slot_grad = jnp.dot(d_gate, gate_mat.T, preferred_element_type=jnp.float32) + jnp.dot(d_up, up_mat.T, preferred_element_type=jnp.float32)
    return slot_grad, grad_gate_e, grad_up_e, d_down


def reference(grad_out, routes, route_probs, dispatched, w_gate, w_up, w_down):
    groups = N_EXPERT
    window = N_EXPERT // 2
    row_count = N_EXPERT * CAPS
    gate_blocks = w_gate.reshape(D, window, F).transpose(1, 0, 2)
    up_blocks = w_up.reshape(D, window, F).transpose(1, 0, 2)
    down_blocks = w_down.reshape(window, F, D)
    inputs = dispatched.reshape(MB * N_DP, groups, row_count, D)[:, ::2]
    out_grads = grad_out.reshape(MB * N_DP, groups * TOK_DEV, D)
    route_ids = routes.reshape(MB * N_DP, groups, TOK_DEV * TOPK)
    weights_all = route_probs.reshape(MB * N_DP, groups, TOK_DEV, TOPK)

    def group_step(totals, pieces):
        group_x, group_dy, group_ids, group_probs = pieces
        hitting = (group_ids[:, :, None] == jnp.arange(window, dtype=jnp.int32)[None, None, :]).astype(jnp.int32)
        ranking = jnp.sum((jnp.cumsum(hitting, axis=1) - 1) * hitting, axis=2)
        source = jnp.arange(groups, dtype=jnp.int32)[:, None]
        where_to = jnp.where(group_ids < window, group_ids * row_count + source * CAPS + ranking, window * row_count).astype(jnp.int32)
        scaled = (group_probs[..., None].astype(jnp.float32) * group_dy.reshape(groups, TOK_DEV, 1, D).astype(jnp.float32)).astype(jnp.bfloat16)
        buffer = jnp.zeros((window * row_count + 1, D), jnp.bfloat16).at[where_to.reshape(-1)].set(scaled.reshape(-1, D))
        slot_grads = buffer[:-1].reshape(window, row_count, D)

        def one_expert(packed):
            return expert_backward(packed[0], packed[1], packed[2], packed[3], packed[4])

        slot_grad, grad_gate_e, grad_up_e, d_down = lax.map(one_expert, (group_x, slot_grads, gate_blocks, up_blocks, down_blocks))
        padded = jnp.concatenate([slot_grad.reshape(window * row_count, D), jnp.zeros((1, D), jnp.float32)], axis=0)
        per_route = padded[where_to.reshape(-1)].reshape(groups * TOK_DEV, TOPK, D)
        grad_tokens = jnp.sum(per_route, axis=1).astype(jnp.bfloat16)
        totals = (totals[0] + grad_gate_e, totals[1] + grad_up_e, totals[2] + d_down)
        return totals, grad_tokens

    start = (jnp.zeros((window, D, F), jnp.float32), jnp.zeros((window, D, F), jnp.float32), jnp.zeros((window, D, F), jnp.float32))
    totals, grad_tokens = lax.scan(group_step, start, (inputs, out_grads, route_ids, weights_all))
    factor = 1.0 / (MB * N_DP)
    grad_gate = (totals[0] * factor).transpose(1, 0, 2).reshape(D, window * F)
    grad_up = (totals[1] * factor).transpose(1, 0, 2).reshape(D, window * F)
    grad_down_t = (totals[2] * factor).transpose(1, 0, 2).reshape(D, window * F)
    grad_in = grad_tokens.reshape(MB, N_DP * groups * TOK_DEV, D)
    return grad_in, grad_gate, grad_up, grad_down_t
```

```python
import jax
import jax.numpy as jnp
from jax import lax
from jax.experimental import pallas as pl
from jax.experimental.pallas import tpu as pltpu
from jax.sharding import Mesh
from jax.sharding import PartitionSpec as P

TOPK = 8
CAPS = 8
DP = ("zl", "y", "core")
DP_CHIPS = ("zl", "y")
EXPERT = ("x", "zq", "zp")
ALL_DP = DP + EXPERT
VMEM = pl.BlockSpec(memory_space=pltpu.VMEM)


def dot(left, right, contract):
    return lax.dot_general(
        left, right, ((contract[:1], contract[1:]), ((), ())), preferred_element_type=jnp.float32
    )


def call(body, outs, flops, name, specs):
    return pl.pallas_call(
        body,
        out_shape=outs,
        in_specs=specs,
        out_specs=jax.tree.map(lambda _: VMEM, outs),
        name=name,
        compiler_params=pltpu.CompilerParams(vmem_limit_bytes=20 * 1024 * 1024),
        cost_estimate=pl.CostEstimate(flops=flops, bytes_accessed=4 << 20, transcendentals=0),
    )


def route_body(ids_ref, probs_ref, grad_ref, send_ref, pick_ref):
    micro, _, tokens = ids_ref.shape
    holders = send_ref.shape[0]
    rows = holders * CAPS
    row = lax.broadcasted_iota(jnp.int32, (rows, tokens), 0)
    expert = row // (2 * CAPS)
    slot = (row % CAPS).astype(jnp.float32)
    earlier = (
        lax.broadcasted_iota(jnp.int32, (tokens, tokens), 0)
        < lax.broadcasted_iota(jnp.int32, (tokens, tokens), 1)
    ).astype(jnp.bfloat16)
    for m in range(micro):
        weight = jnp.zeros((rows, tokens), jnp.float32)
        live = jnp.zeros((rows, tokens), jnp.float32)
        for k in range(TOPK):
            named = ids_ref[m, k : k + 1, :] == expert
            weight = jnp.where(named, probs_ref[m, k : k + 1, :].astype(jnp.float32), weight)
            live = jnp.where(named, 1.0, live)
        rank = dot(live.astype(jnp.bfloat16), earlier, (1, 0))
        chosen = jnp.logical_and(live > 0.0, rank == slot)
        pick_ref[m] = chosen.astype(jnp.bfloat16)
        scaled = dot(jnp.where(chosen, weight, 0.0).astype(jnp.bfloat16), grad_ref[m], (1, 0))
        send_ref[:, m * CAPS : (m + 1) * CAPS, :] = scaled.astype(jnp.bfloat16).reshape(
            holders, CAPS, -1
        )


def forward_body(x_ref, gate_w_ref, up_w_ref, hidden_ref, to_up_ref, to_gate_ref):
    for m in range(x_ref.shape[0]):
        x = x_ref[m]
        gate = dot(x, gate_w_ref[...], (1, 0))
        up = dot(x, up_w_ref[...], (1, 0))
        sigmoid = jax.nn.sigmoid(gate)
        activated = gate * sigmoid
        hidden_ref[m] = (activated * up).astype(jnp.bfloat16)
        to_up_ref[m] = activated
        to_gate_ref[m] = up * sigmoid * (1.0 + gate * (1.0 - sigmoid))


def slot_body(
    got_ref, to_up_ref, to_gate_ref, gate_w_ref, up_w_ref, down_w_ref, back_ref, d_gate_ref, d_up_ref
):
    holders = got_ref.shape[0]
    for m in range(to_up_ref.shape[0]):
        part = slice(m * CAPS, (m + 1) * CAPS)
        scaled = got_ref[:, part, :].reshape(holders * CAPS, -1)
        d_hidden = dot(scaled, down_w_ref[...], (1, 1))
        d_gate = (d_hidden * to_gate_ref[m]).astype(jnp.bfloat16)
        d_up = (d_hidden * to_up_ref[m]).astype(jnp.bfloat16)
        d_gate_ref[m] = d_gate
        d_up_ref[m] = d_up
        back = dot(d_gate, gate_w_ref[...], (1, 1)) + dot(d_up, up_w_ref[...], (1, 1))
        back_ref[:, part, :] = back.astype(jnp.bfloat16).reshape(holders, CAPS, -1)


def weight_body(core_ref, x_ref, got_ref, hidden_ref, d_gate_ref, d_up_ref, keep_ref, give_ref, all_ref):
    micro, slots, width = x_ref.shape
    chips, rows, _ = keep_ref.shape
    cols = hidden_ref.shape[2]
    core = core_ref[0]
    x = x_ref[...].reshape(micro * slots, width)
    got = jnp.concatenate(
        [
            got_ref[:, m * CAPS : (m + 1) * CAPS, :].reshape(slots, width)
            for m in range(micro)
        ],
        axis=0,
    )
    terms = ((x, d_gate_ref), (x, d_up_ref), (got, hidden_ref))
    for k, (left, right_ref) in enumerate(terms):
        total = dot(left, right_ref[...].reshape(micro * slots, cols), (0, 0))
        all_ref[:, :, :, k * cols : (k + 1) * cols] = total.reshape(chips, 2, rows, cols)
    keep_ref[...] = all_ref[:, pl.ds(core, 1)].reshape(keep_ref.shape)
    give_ref[...] = all_ref[:, pl.ds(1 - core, 1)].reshape(give_ref.shape)


def mix_body(pick_ref, back_ref, out_ref):
    holders = back_ref.shape[0]
    for m in range(pick_ref.shape[0]):
        rows = back_ref[:, m * CAPS : (m + 1) * CAPS, :].reshape(holders * CAPS, -1)
        out_ref[m] = dot(pick_ref[m], rows, (0, 0)).astype(jnp.bfloat16)


def total_body(factor, terms_ref, gate_ref, up_ref, down_ref):
    total = terms_ref[0].astype(jnp.float32)
    for k in range(1, terms_ref.shape[0]):
        total = total + terms_ref[k].astype(jnp.float32)
    total = total * factor
    cols = gate_ref.shape[1]
    gate_ref[...] = total[:, :cols]
    up_ref[...] = total[:, cols : 2 * cols]
    down_ref[...] = total[:, 2 * cols :]


def per_device(grad_out, routes, route_probs, dispatched, w_gate, w_up, w_down):
    micro, tokens, width = grad_out.shape
    slots = dispatched.shape[1]
    cols = w_gate.shape[1]
    holders = lax.axis_size("x") * lax.axis_size("zq") * lax.axis_size("zp")
    chips = lax.axis_size("zl") * lax.axis_size("y")
    rows = width // (2 * chips)
    bf16, f32 = jnp.bfloat16, jnp.float32
    shape = jax.ShapeDtypeStruct

    send, pick = call(
        route_body,
        (
            shape((holders, micro * CAPS, width), bf16),
            shape((micro, holders * CAPS, tokens), bf16),
        ),
        1 << 27,
        "route",
        [VMEM] * 3,
    )(jnp.swapaxes(routes, 1, 2), jnp.swapaxes(route_probs, 1, 2), grad_out)
    with jax.named_scope("dispatch"):
        got = lax.all_to_all(send, EXPERT, 0, 0, tiled=True)
    hidden, to_up, to_gate = call(
        forward_body,
        (
            shape((micro, slots, cols), bf16),
            shape((micro, slots, cols), f32),
            shape((micro, slots, cols), f32),
        ),
        1 << 30,
        "forward",
        [VMEM] * 3,
    )(dispatched, w_gate, w_up)
    back_send, d_gate, d_up = call(
        slot_body,
        (
            shape((holders, micro * CAPS, width), bf16),
            shape((micro, slots, cols), bf16),
            shape((micro, slots, cols), bf16),
        ),
        1 << 30,
        "slots",
        [VMEM] * 6,
    )(got, to_up, to_gate, w_gate, w_up, w_down)
    with jax.named_scope("back"):
        back = lax.all_to_all(back_send, EXPERT, 0, 0, tiled=True)
    core = lax.axis_index("core").astype(jnp.int32).reshape(1)
    keep, give = pl.pallas_call(
        weight_body,
        out_shape=(shape((chips, rows, 3 * cols), f32), shape((chips, rows, 3 * cols), f32)),
        in_specs=[pl.BlockSpec(memory_space=pltpu.SMEM)] + [VMEM] * 5,
        out_specs=(VMEM, VMEM),
        scratch_shapes=[pltpu.VMEM((chips, 2, rows, 3 * cols), f32)],
        name="weights",
        compiler_params=pltpu.CompilerParams(vmem_limit_bytes=20 * 1024 * 1024),
        cost_estimate=pl.CostEstimate(flops=1 << 30, bytes_accessed=8 << 20, transcendentals=0),
    )(core, dispatched, got, hidden, d_gate, d_up)
    with jax.named_scope("cores"):
        other = lax.ppermute(give, "core", [(0, 1), (1, 0)])
    chip_sum = (keep + other).astype(bf16)
    with jax.named_scope("reduce"):
        terms = lax.all_to_all(chip_sum, DP_CHIPS, 0, 0, tiled=True)
    grad_in = call(
        mix_body, shape((micro, tokens, width), bf16), 1 << 27, "mix", [VMEM] * 2
    )(pick, back)
    factor = 1.0 / (micro * chips * 2)
    grads = call(
        lambda *refs: total_body(factor, *refs),
        tuple(shape((rows, cols), f32) for _ in range(3)),
        1 << 20,
        "total",
        [VMEM],
    )(terms)
    return (grad_in, *grads)


def solution(mesh):
    fine = Mesh(mesh.devices.reshape(2, 8, 2, 4, 2, 2), DP + EXPERT)
    tokens = P(None, ALL_DP, None)
    return jax.shard_map(
        per_device,
        mesh=fine,
        in_specs=(tokens, tokens, tokens, tokens, P(None, EXPERT), P(None, EXPERT), P(EXPERT, None)),
        out_specs=(tokens, P(DP, EXPERT), P(DP, EXPERT), P(DP, EXPERT)),
        check_vma=False,
    )
```

```python
import jax
import jax.numpy as jnp
from jax import lax
from jax.experimental import pallas as pl
from jax.experimental.pallas import tpu as pltpu
from jax.sharding import Mesh
from jax.sharding import PartitionSpec as P

TOPK = 8
CAPS = 8
DP = ("zl", "y", "core")
EXPERT = ("x", "zq", "zp")
STAGES = (("core", 1), ("y", 1), ("y", 2))
LAST = (4, 8, 12)
ALL_DP = DP + EXPERT
VMEM = pl.BlockSpec(memory_space=pltpu.VMEM)
HBM = pl.BlockSpec(memory_space=pltpu.HBM)


def dot(left, right, contract):
    return lax.dot_general(
        left, right, ((contract[:1], contract[1:]), ((), ())), preferred_element_type=jnp.float32
    )


def call(body, outs, flops, specs, scratch=(), to_hbm=0, limit=20):
    return pl.pallas_call(
        body,
        out_shape=outs,
        in_specs=specs,
        out_specs=tuple(HBM if k < to_hbm else VMEM for k in range(len(outs))),
        scratch_shapes=list(scratch),
        compiler_params=pltpu.CompilerParams(vmem_limit_bytes=limit * 1024 * 1024),
        cost_estimate=pl.CostEstimate(flops=flops, bytes_accessed=4 << 20, transcendentals=0),
    )


def route_body(
    ids_hbm,
    probs_hbm,
    grad_hbm,
    send_hbm,
    pick_ref,
    ids_ref,
    probs_ref,
    grad_ref,
    send_ref,
    sems,
    out_sems,
):
    copies = [
        pltpu.make_async_copy(source, goal, sems.at[k])
        for k, (source, goal) in enumerate(
            ((ids_hbm, ids_ref), (probs_hbm, probs_ref), (grad_hbm, grad_ref))
        )
    ]
    for copy in copies:
        copy.start()
    micro, _, tokens = ids_ref.shape
    holders = send_ref.shape[1]
    rows = holders * CAPS
    row = lax.broadcasted_iota(jnp.int32, (rows, tokens), 0)
    expert = row // (2 * CAPS)
    slot = (row % CAPS).astype(jnp.float32)
    earlier = (
        lax.broadcasted_iota(jnp.int32, (tokens, tokens), 0)
        < lax.broadcasted_iota(jnp.int32, (tokens, tokens), 1)
    ).astype(jnp.bfloat16)
    for copy in copies[:2]:
        copy.wait()
    weights = []
    for m in range(micro):
        weight = jnp.zeros((rows, tokens), jnp.float32)
        live = jnp.zeros((rows, tokens), jnp.float32)
        for k in range(TOPK):
            named = ids_ref[m, k : k + 1, :] == expert
            weight = jnp.where(named, probs_ref[m, k : k + 1, :].astype(jnp.float32), weight)
            live = jnp.where(named, 1.0, live)
        rank = dot(live.astype(jnp.bfloat16), earlier, (1, 0))
        chosen = jnp.logical_and(live > 0.0, rank == slot)
        pick_ref[m] = chosen.astype(jnp.bfloat16)
        weights.append(jnp.where(chosen, weight, 0.0).astype(jnp.bfloat16))
    copies[2].wait()
    puts = []
    for m in range(micro):
        scaled = dot(weights[m], grad_ref[m], (1, 0))
        send_ref[m] = scaled.astype(jnp.bfloat16).reshape(holders, CAPS, -1)
        put = pltpu.make_async_copy(
            send_ref.at[m], send_hbm.at[:, pl.ds(m * CAPS, CAPS), :], out_sems.at[m]
        )
        put.start()
        puts.append(put)
    for put in puts:
        put.wait()


def weight_body(
    got_ref,
    x_ref,
    gate_w_ref,
    up_w_ref,
    down_w_ref,
    d_gate_ref,
    d_up_ref,
    keep_ref,
    give_ref,
    got_all_ref,
    all_ref,
):
    micro, slots, width = x_ref.shape
    pieces, rows, _ = all_ref.shape
    cols = gate_w_ref.shape[1]
    x = x_ref[...].reshape(micro * slots, width)
    for m in range(micro):
        got_all_ref[m * slots : (m + 1) * slots] = got_ref[
            :, m * CAPS : (m + 1) * CAPS, :
        ].reshape(slots, width)
    gate = dot(x, gate_w_ref[...], (1, 0))
    up = dot(x, up_w_ref[...], (1, 0))
    sigmoid = jax.nn.sigmoid(gate)
    activated = gate * sigmoid
    hidden = (activated * up).astype(jnp.bfloat16)
    to_gate = up * sigmoid * (1.0 + gate * (1.0 - sigmoid))
    d_hidden = dot(got_all_ref[...], down_w_ref[...], (1, 1))
    d_gate_ref[...] = (d_hidden * to_gate).astype(jnp.bfloat16)
    d_up_ref[...] = (d_hidden * activated).astype(jnp.bfloat16)
    terms = ((x, d_gate_ref[...]), (x, d_up_ref[...]), (got_all_ref[...], hidden))
    for k, (left, right) in enumerate(terms):
        total = dot(left, right, (0, 0))
        all_ref[:, :, k * cols : (k + 1) * cols] = total.reshape(pieces, rows, cols)
    me = lax.axis_index(DP)
    for k in range(pieces // 2):
        keep_ref[k] = all_ref[me ^ (2 * k)]
        give_ref[k] = all_ref[me ^ (2 * k + 1)].astype(jnp.bfloat16)


def slot_body(d_gate_ref, d_up_ref, gate_w_ref, up_w_ref, back_hbm, back_ref, sems):
    micro, holders, _, width = back_ref.shape
    slots = holders * CAPS
    puts = []
    for m in range(micro):
        rows = slice(m * slots, (m + 1) * slots)
        back = dot(d_gate_ref[rows], gate_w_ref[...], (1, 1)) + dot(
            d_up_ref[rows], up_w_ref[...], (1, 1)
        )
        back_ref[m] = back.astype(jnp.bfloat16).reshape(holders, CAPS, width)
        put = pltpu.make_async_copy(
            back_ref.at[m], back_hbm.at[:, pl.ds(m * CAPS, CAPS), :], sems.at[m]
        )
        put.start()
        puts.append(put)
    for put in puts:
        put.wait()


def halve_body(keep_ref, other_ref, next_keep_ref, next_give_ref):
    for k in range(next_keep_ref.shape[0]):
        next_keep_ref[k] = keep_ref[2 * k] + other_ref[2 * k].astype(jnp.float32)
        next_give_ref[k] = (
            keep_ref[2 * k + 1] + other_ref[2 * k + 1].astype(jnp.float32)
        ).astype(jnp.bfloat16)


def spread_body(keep_ref, other_ref, next_keep_ref, *give_refs):
    next_keep_ref[...] = keep_ref[0] + other_ref[0].astype(jnp.float32)
    for k, give_ref in enumerate(give_refs, 1):
        give_ref[...] = (keep_ref[k] + other_ref[k].astype(jnp.float32)).astype(jnp.bfloat16)


def mix_body(pick_ref, back_ref, out_ref):
    holders = back_ref.shape[0]
    for m in range(pick_ref.shape[0]):
        rows = back_ref[:, m * CAPS : (m + 1) * CAPS, :].reshape(holders * CAPS, -1)
        out_ref[m] = dot(pick_ref[m], rows, (0, 0)).astype(jnp.bfloat16)


def total_body(factor, keep_ref, *refs):
    other_refs, out_refs = refs[:-3], refs[-3:]
    cols = out_refs[0].shape[1]
    total = keep_ref[...]
    for other_ref in other_refs:
        total = total + other_ref[...].astype(jnp.float32)
    total = total * factor
    for k, out_ref in enumerate(out_refs):
        out_ref[...] = total[:, k * cols : (k + 1) * cols]


def flipped(size, flip):
    return [(i, i ^ flip) for i in range(size)]


def per_device(grad_out, routes, route_probs, dispatched, w_gate, w_up, w_down):
    micro, tokens, width = grad_out.shape
    slots = dispatched.shape[1]
    cols = w_gate.shape[1]
    holders = lax.axis_size(EXPERT)
    pieces = lax.axis_size(DP)
    rows = width // pieces
    bf16, f32 = jnp.bfloat16, jnp.float32
    shape = jax.ShapeDtypeStruct

    send, pick = call(
        route_body,
        (
            shape((holders, micro * CAPS, width), bf16),
            shape((micro, holders * CAPS, tokens), bf16),
        ),
        1 << 27,
        [HBM] * 3,
        [
            pltpu.VMEM((micro, TOPK, tokens), jnp.int32),
            pltpu.VMEM((micro, TOPK, tokens), bf16),
            pltpu.VMEM(grad_out.shape, bf16),
            pltpu.VMEM((micro, holders, CAPS, width), bf16),
            pltpu.SemaphoreType.DMA((3,)),
            pltpu.SemaphoreType.DMA((micro,)),
        ],
        1,
        60,
    )(jnp.swapaxes(routes, 1, 2), jnp.swapaxes(route_probs, 1, 2), grad_out)
    got = lax.all_to_all(send, EXPERT, 0, 0, tiled=True)
    def lot(count):
        return count, rows, 3 * cols

    d_gate, d_up, keep, give = call(
        weight_body,
        (
            shape((micro * slots, cols), bf16),
            shape((micro * slots, cols), bf16),
            shape(lot(pieces // 2), f32),
            shape(lot(pieces // 2), bf16),
        ),
        1 << 31,
        [VMEM] * 5,
        [pltpu.VMEM((micro * slots, width), bf16), pltpu.VMEM(lot(pieces), f32)],
    )(got, dispatched, w_gate, w_up, w_down)
    (back_send,) = call(
        slot_body,
        (shape((holders, micro * CAPS, width), bf16),),
        1 << 30,
        [VMEM] * 4,
        [
            pltpu.VMEM((micro, holders, CAPS, width), bf16),
            pltpu.SemaphoreType.DMA((micro,)),
        ],
        1,
    )(d_gate, d_up, w_gate, w_up)
    back = lax.all_to_all(back_send, EXPERT, 0, 0, tiled=True)
    for axis, flip in STAGES:
        other = lax.ppermute(give, axis, flipped(lax.axis_size(axis), flip))
        if (axis, flip) == STAGES[-1]:
            break
        half = lot(keep.shape[0] // 2)
        keep, give = call(
            halve_body, (shape(half, f32), shape(half, bf16)), 1 << 20, [VMEM] * 2
        )(keep, other)
    keep, *gives = call(
        spread_body,
        (shape(lot(1)[1:], f32), *[shape(lot(1)[1:], bf16)] * len(LAST)),
        1 << 20,
        [VMEM] * 2,
    )(keep, other)
    others = []
    for give, flip in zip(gives, LAST):
        others.append(lax.ppermute(give, ("zl", "y"), flipped(lax.axis_size(("zl", "y")), flip)))
    (grad_in,) = call(
        mix_body, (shape((micro, tokens, width), bf16),), 1 << 27, [VMEM] * 2
    )(pick, back)
    factor = 1.0 / (micro * pieces)
    grads = call(
        lambda *refs: total_body(factor, *refs),
        tuple(shape((rows, cols), f32) for _ in range(3)),
        1 << 20,
        [VMEM] * (1 + len(others)),
    )(keep, *others)
    return (grad_in, *grads)


def solution(mesh):
    fine = Mesh(mesh.devices.reshape(2, 8, 2, 4, 2, 2), DP + EXPERT)
    tokens = P(None, ALL_DP, None)
    return jax.shard_map(
        per_device,
        mesh=fine,
        in_specs=(tokens, tokens, tokens, tokens, P(None, EXPERT), P(None, EXPERT), P(EXPERT, None)),
        out_specs=(tokens, P(DP, EXPERT), P(DP, EXPERT), P(DP, EXPERT)),
        check_vma=False,
    )
```

```python
import jax
import jax.numpy as jnp
from jax import lax
from jax.experimental import pallas as pl
from jax.experimental.pallas import tpu as pltpu
from jax.sharding import Mesh
from jax.sharding import PartitionSpec as P

TOPK = 8
CAPS = 8
DP = ("zl", "y", "core")
EXPERT = ("x", "zq", "zp")
ALL_DP = DP + EXPERT


def near(index):
    return index ^ 1


def after(index):
    return (((index + 1) ^ 1) - 1) & 7


def far(index):
    return index ^ 3 ^ (((index ^ (index >> 1)) & 1) << 2)


STAGES = (("core", near), ("y", near), ("y", after), ("y", far), ("zl", near))
VMEM = pl.BlockSpec(memory_space=pltpu.VMEM)
HBM = pl.BlockSpec(memory_space=pltpu.HBM)


def dot(left, right, contract):
    return lax.dot_general(
        left, right, ((contract[:1], contract[1:]), ((), ())), preferred_element_type=jnp.float32
    )


def call(body, outs, flops, specs, scratch=(), to_hbm=0, limit=20):
    return pl.pallas_call(
        body,
        out_shape=outs,
        in_specs=specs,
        out_specs=tuple(HBM if k < to_hbm else VMEM for k in range(len(outs))),
        scratch_shapes=list(scratch),
        compiler_params=pltpu.CompilerParams(vmem_limit_bytes=limit * 1024 * 1024),
        cost_estimate=pl.CostEstimate(flops=flops, bytes_accessed=4 << 20, transcendentals=0),
    )


def route_body(
    ids_hbm,
    probs_hbm,
    grad_hbm,
    send_hbm,
    pick_ref,
    ids_ref,
    probs_ref,
    grad_ref,
    send_ref,
    sems,
    out_sems,
):
    copies = [
        pltpu.make_async_copy(source, goal, sems.at[k])
        for k, (source, goal) in enumerate(
            ((ids_hbm, ids_ref), (probs_hbm, probs_ref), (grad_hbm, grad_ref))
        )
    ]
    for copy in copies:
        copy.start()
    micro, _, tokens = ids_ref.shape
    holders = send_ref.shape[1]
    rows = holders * CAPS
    row = lax.broadcasted_iota(jnp.int32, (rows, tokens), 0)
    expert = row // (2 * CAPS)
    slot = (row % CAPS).astype(jnp.float32)
    earlier = (
        lax.broadcasted_iota(jnp.int32, (tokens, tokens), 0)
        < lax.broadcasted_iota(jnp.int32, (tokens, tokens), 1)
    ).astype(jnp.bfloat16)
    for copy in copies[:2]:
        copy.wait()
    weights = []
    for m in range(micro):
        weight = jnp.zeros((rows, tokens), jnp.float32)
        live = jnp.zeros((rows, tokens), jnp.float32)
        for k in range(TOPK):
            named = ids_ref[m, k : k + 1, :] == expert
            weight = jnp.where(named, probs_ref[m, k : k + 1, :].astype(jnp.float32), weight)
            live = jnp.where(named, 1.0, live)
        rank = dot(live.astype(jnp.bfloat16), earlier, (1, 0))
        chosen = jnp.logical_and(live > 0.0, rank == slot)
        pick_ref[m] = chosen.astype(jnp.bfloat16)
        weights.append(jnp.where(chosen, weight, 0.0).astype(jnp.bfloat16))
    copies[2].wait()
    puts = []
    for m in range(micro):
        scaled = dot(weights[m], grad_ref[m], (1, 0))
        send_ref[m] = scaled.astype(jnp.bfloat16).reshape(holders, CAPS, -1)
        put = pltpu.make_async_copy(
            send_ref.at[m], send_hbm.at[:, pl.ds(m * CAPS, CAPS), :], out_sems.at[m]
        )
        put.start()
        puts.append(put)
    for put in puts:
        put.wait()


def weight_body(
    got_ref,
    x_ref,
    gate_w_ref,
    up_w_ref,
    down_w_ref,
    d_gate_ref,
    d_up_ref,
    keep_ref,
    give_ref,
    got_all_ref,
    all_ref,
):
    micro, slots, width = x_ref.shape
    pieces, rows, _ = all_ref.shape
    cols = gate_w_ref.shape[1]
    x = x_ref[...].reshape(micro * slots, width)
    for m in range(micro):
        got_all_ref[m * slots : (m + 1) * slots] = got_ref[
            :, m * CAPS : (m + 1) * CAPS, :
        ].reshape(slots, width)
    gate = dot(x, gate_w_ref[...], (1, 0))
    up = dot(x, up_w_ref[...], (1, 0))
    sigmoid = jax.nn.sigmoid(gate)
    activated = gate * sigmoid
    hidden = (activated * up).astype(jnp.bfloat16)
    to_gate = up * sigmoid * (1.0 + gate * (1.0 - sigmoid))
    d_hidden = dot(got_all_ref[...], down_w_ref[...], (1, 1))
    d_gate_ref[...] = (d_hidden * to_gate).astype(jnp.bfloat16)
    d_up_ref[...] = (d_hidden * activated).astype(jnp.bfloat16)
    terms = ((x, d_gate_ref[...]), (x, d_up_ref[...]), (got_all_ref[...], hidden))
    for k, (left, right) in enumerate(terms):
        total = dot(left, right, (0, 0))
        all_ref[:, :, k * cols : (k + 1) * cols] = total.reshape(pieces, rows, cols)
    for k in range(pieces // 2):
        place = {axis: lax.axis_index(axis) for axis in DP}
        for bit, (axis, partner) in enumerate(STAGES[1:]):
            if k >> bit & 1:
                place[axis] = partner(place[axis])
        chip = (place["zl"] * lax.axis_size("y") + place["y"]) * 2
        keep_ref[k] = all_ref[chip + place["core"]]
        give_ref[k] = all_ref[chip + near(place["core"])].astype(jnp.bfloat16)


def slot_body(d_gate_ref, d_up_ref, gate_w_ref, up_w_ref, back_hbm, back_ref, sems):
    micro, holders, _, width = back_ref.shape
    slots = holders * CAPS
    puts = []
    for m in range(micro):
        rows = slice(m * slots, (m + 1) * slots)
        back = dot(d_gate_ref[rows], gate_w_ref[...], (1, 1)) + dot(
            d_up_ref[rows], up_w_ref[...], (1, 1)
        )
        back_ref[m] = back.astype(jnp.bfloat16).reshape(holders, CAPS, width)
        put = pltpu.make_async_copy(
            back_ref.at[m], back_hbm.at[:, pl.ds(m * CAPS, CAPS), :], sems.at[m]
        )
        put.start()
        puts.append(put)
    for put in puts:
        put.wait()


def halve_body(keep_ref, other_ref, next_keep_ref, next_give_ref):
    for k in range(next_keep_ref.shape[0]):
        next_keep_ref[k] = keep_ref[2 * k] + other_ref[2 * k].astype(jnp.float32)
        next_give_ref[k] = (
            keep_ref[2 * k + 1] + other_ref[2 * k + 1].astype(jnp.float32)
        ).astype(jnp.bfloat16)


def mix_body(pick_ref, back_ref, out_ref):
    holders = back_ref.shape[0]
    for m in range(pick_ref.shape[0]):
        rows = back_ref[:, m * CAPS : (m + 1) * CAPS, :].reshape(holders * CAPS, -1)
        out_ref[m] = dot(pick_ref[m], rows, (0, 0)).astype(jnp.bfloat16)


def total_body(factor, keep_ref, other_ref, *out_refs):
    cols = out_refs[0].shape[1]
    total = (keep_ref[0] + other_ref[0].astype(jnp.float32)) * factor
    for k, out_ref in enumerate(out_refs):
        out_ref[...] = total[:, k * cols : (k + 1) * cols]


def per_device(grad_out, routes, route_probs, dispatched, w_gate, w_up, w_down):
    micro, tokens, width = grad_out.shape
    slots = dispatched.shape[1]
    cols = w_gate.shape[1]
    holders = lax.axis_size(EXPERT)
    pieces = lax.axis_size(DP)
    rows = width // pieces
    bf16, f32 = jnp.bfloat16, jnp.float32
    shape = jax.ShapeDtypeStruct

    send, pick = call(
        route_body,
        (
            shape((holders, micro * CAPS, width), bf16),
            shape((micro, holders * CAPS, tokens), bf16),
        ),
        1 << 27,
        [HBM] * 3,
        [
            pltpu.VMEM((micro, TOPK, tokens), jnp.int32),
            pltpu.VMEM((micro, TOPK, tokens), bf16),
            pltpu.VMEM(grad_out.shape, bf16),
            pltpu.VMEM((micro, holders, CAPS, width), bf16),
            pltpu.SemaphoreType.DMA((3,)),
            pltpu.SemaphoreType.DMA((micro,)),
        ],
        1,
        60,
    )(jnp.swapaxes(routes, 1, 2), jnp.swapaxes(route_probs, 1, 2), grad_out)
    got = lax.all_to_all(send, EXPERT, 0, 0, tiled=True)
    def lot(count):
        return count, rows, 3 * cols

    d_gate, d_up, keep, give = call(
        weight_body,
        (
            shape((micro * slots, cols), bf16),
            shape((micro * slots, cols), bf16),
            shape(lot(pieces // 2), f32),
            shape(lot(pieces // 2), bf16),
        ),
        1 << 31,
        [VMEM] * 5,
        [pltpu.VMEM((micro * slots, width), bf16), pltpu.VMEM(lot(pieces), f32)],
    )(got, dispatched, w_gate, w_up, w_down)
    (back_send,) = call(
        slot_body,
        (shape((holders, micro * CAPS, width), bf16),),
        1 << 30,
        [VMEM] * 4,
        [
            pltpu.VMEM((micro, holders, CAPS, width), bf16),
            pltpu.SemaphoreType.DMA((micro,)),
        ],
        1,
    )(d_gate, d_up, w_gate, w_up)
    back = lax.all_to_all(back_send, EXPERT, 0, 0, tiled=True)
    for stage, (axis, partner) in enumerate(STAGES):
        goals = [(i, partner(i)) for i in range(lax.axis_size(axis))]
        other = lax.ppermute(give, axis, goals)
        if stage == len(STAGES) - 1:
            break
        half = lot(keep.shape[0] // 2)
        keep, give = call(
            halve_body, (shape(half, f32), shape(half, bf16)), 1 << 20, [VMEM] * 2
        )(keep, other)
    (grad_in,) = call(
        mix_body, (shape((micro, tokens, width), bf16),), 1 << 27, [VMEM] * 2
    )(pick, back)
    factor = 1.0 / (micro * pieces)
    grads = call(
        lambda *refs: total_body(factor, *refs),
        tuple(shape((rows, cols), f32) for _ in range(3)),
        1 << 20,
        [VMEM] * 2,
    )(keep, other)
    return (grad_in, *grads)


def solution(mesh):
    fine = Mesh(mesh.devices.reshape(2, 8, 2, 4, 2, 2), DP + EXPERT)
    tokens = P(None, ALL_DP, None)
    return jax.shard_map(
        per_device,
        mesh=fine,
        in_specs=(tokens, tokens, tokens, tokens, P(None, EXPERT), P(None, EXPERT), P(EXPERT, None)),
        out_specs=(tokens, P(DP, EXPERT), P(DP, EXPERT), P(DP, EXPERT)),
        check_vma=False,
    )
```

```python
import jax
import jax.numpy as jnp
from jax import lax
from jax.experimental import pallas as pl
from jax.experimental.pallas import tpu as pltpu
from jax.sharding import Mesh
from jax.sharding import PartitionSpec as P

TOPK = 8
CAPS = 8
DP = ("zl", "y", "core")
EXPERT = ("x", "zq", "zp")
ALL_DP = DP + EXPERT


def near(index):
    return index ^ 1


def plus(index):
    return (index + 2) & 7


def minus(index):
    return (index + 6) & 7


def cross(index):
    return (index + 5 - 2 * (index & 1)) & 7


TURNS = (cross, plus, minus)
VMEM = pl.BlockSpec(memory_space=pltpu.VMEM)
HBM = pl.BlockSpec(memory_space=pltpu.HBM)


def dot(left, right, contract):
    return lax.dot_general(
        left, right, ((contract[:1], contract[1:]), ((), ())), preferred_element_type=jnp.float32
    )


def call(body, outs, flops, specs, scratch=(), to_hbm=0, limit=20):
    return pl.pallas_call(
        body,
        out_shape=outs,
        in_specs=specs,
        out_specs=tuple(HBM if k < to_hbm else VMEM for k in range(len(outs))),
        scratch_shapes=list(scratch),
        compiler_params=pltpu.CompilerParams(vmem_limit_bytes=limit * 1024 * 1024),
        cost_estimate=pl.CostEstimate(flops=flops, bytes_accessed=4 << 20, transcendentals=0),
    )


def route_body(
    ids_hbm,
    probs_hbm,
    grad_hbm,
    send_hbm,
    pick_hbm,
    ids_ref,
    probs_ref,
    grad_ref,
    send_ref,
    pick_ref,
    sems,
    out_sems,
):
    copies = [
        pltpu.make_async_copy(source, goal, sems.at[k])
        for k, (source, goal) in enumerate(
            ((ids_hbm, ids_ref), (probs_hbm, probs_ref), (grad_hbm, grad_ref))
        )
    ]
    for copy in copies:
        copy.start()
    micro, _, tokens = ids_ref.shape
    holders, _, width = send_ref.shape[1:]
    rows = holders // 2 * CAPS
    row = lax.broadcasted_iota(jnp.int32, (rows, tokens), 0)
    expert = row // CAPS
    slot = (row % CAPS).astype(jnp.float32)
    earlier = (
        lax.broadcasted_iota(jnp.int32, (tokens, tokens), 0)
        < lax.broadcasted_iota(jnp.int32, (tokens, tokens), 1)
    ).astype(jnp.bfloat16)
    for copy in copies[:2]:
        copy.wait()
    weights = []
    for m in range(micro):
        weight = jnp.zeros((rows, tokens), jnp.float32)
        live = jnp.zeros((rows, tokens), jnp.float32)
        for k in range(TOPK):
            named = ids_ref[m, k : k + 1, :] == expert
            weight = jnp.where(named, probs_ref[m, k : k + 1, :].astype(jnp.float32), weight)
            live = jnp.where(named, 1.0, live)
        rank = dot(live.astype(jnp.bfloat16), earlier, (1, 0))
        chosen = jnp.logical_and(live > 0.0, rank == slot)
        pick_ref[m] = chosen.astype(jnp.bfloat16)
        weights.append(jnp.where(chosen, weight, 0.0).astype(jnp.bfloat16))
    copies[2].wait()
    puts = []
    for m in range(micro):
        scaled = dot(weights[m], grad_ref[m], (1, 0)).astype(jnp.bfloat16)
        send_ref[m] = jnp.broadcast_to(
            scaled.reshape(holders // 2, 1, CAPS, width), (holders // 2, 2, CAPS, width)
        ).reshape(holders, CAPS, width)
        puts.append(
            pltpu.make_async_copy(
                send_ref.at[m], send_hbm.at[:, pl.ds(m * CAPS, CAPS), :], out_sems.at[m]
            )
        )
        puts[-1].start()
    puts.append(pltpu.make_async_copy(pick_ref, pick_hbm, out_sems.at[micro]))
    puts[-1].start()
    for put in puts:
        put.wait()


def weight_body(
    got_ref,
    x_ref,
    gate_w_ref,
    up_w_ref,
    down_w_ref,
    d_gate_ref,
    d_up_ref,
    keep_ref,
    give_ref,
    got_all_ref,
    all_ref,
):
    micro, slots, width = x_ref.shape
    pieces, rows, _ = all_ref.shape
    cols = gate_w_ref.shape[1]
    x = x_ref[...].reshape(micro * slots, width)
    for m in range(micro):
        got_all_ref[m * slots : (m + 1) * slots] = got_ref[
            :, m * CAPS : (m + 1) * CAPS, :
        ].reshape(slots, width)
    gate = dot(x, gate_w_ref[...], (1, 0))
    up = dot(x, up_w_ref[...], (1, 0))
    sigmoid = jax.nn.sigmoid(gate)
    activated = gate * sigmoid
    hidden = (activated * up).astype(jnp.bfloat16)
    to_gate = up * sigmoid * (1.0 + gate * (1.0 - sigmoid))
    d_hidden = dot(got_all_ref[...], down_w_ref[...], (1, 1))
    d_gate_ref[...] = (d_hidden * to_gate).astype(jnp.bfloat16)
    d_up_ref[...] = (d_hidden * activated).astype(jnp.bfloat16)
    terms = ((x, d_gate_ref[...]), (x, d_up_ref[...]), (got_all_ref[...], hidden))
    for k, (left, right) in enumerate(terms):
        total = dot(left, right, (0, 0))
        all_ref[:, :, k * cols : (k + 1) * cols] = total.reshape(pieces, rows, cols)
    plane, line, core = (lax.axis_index(axis) for axis in DP)
    for k in range(pieces // 2):
        goal = near(line) if k & 1 else line
        goal = TURNS[(k >> 2) - 1](goal) if k >> 2 else goal
        chip = ((plane ^ (k >> 1 & 1)) * lax.axis_size("y") + goal) * 2
        keep_ref[k] = all_ref[chip + core]
        give_ref[k] = all_ref[chip + near(core)].astype(jnp.bfloat16)


def slot_body(d_gate_ref, d_up_ref, gate_w_ref, up_w_ref, back_hbm, back_ref, sems):
    micro, holders, _, width = back_ref.shape
    slots = holders * CAPS
    puts = []
    for m in range(micro):
        rows = slice(m * slots, (m + 1) * slots)
        back = dot(d_gate_ref[rows], gate_w_ref[...], (1, 1)) + dot(
            d_up_ref[rows], up_w_ref[...], (1, 1)
        )
        back_ref[m] = back.astype(jnp.bfloat16).reshape(holders, CAPS, width)
        put = pltpu.make_async_copy(
            back_ref.at[m], back_hbm.at[:, pl.ds(m * CAPS, CAPS), :], sems.at[m]
        )
        put.start()
        puts.append(put)
    for put in puts:
        put.wait()


def halve_body(keep_ref, other_ref, next_keep_ref, next_give_ref):
    for k in range(next_keep_ref.shape[0]):
        next_keep_ref[k] = keep_ref[2 * k] + other_ref[2 * k].astype(jnp.float32)
        next_give_ref[k] = (
            keep_ref[2 * k + 1] + other_ref[2 * k + 1].astype(jnp.float32)
        ).astype(jnp.bfloat16)


def spread_body(keep_ref, other_ref, next_keep_ref, *give_refs):
    for k in range(2):
        turns = [
            keep_ref[2 * t + k] + other_ref[2 * t + k].astype(jnp.float32)
            for t in range(1 + len(give_refs))
        ]
        next_keep_ref[k] = turns[0]
        for give_ref, turn in zip(give_refs, turns[1:]):
            give_ref[k] = turn.astype(jnp.bfloat16)


def gather_body(keep_ref, *refs):
    *other_refs, next_keep_ref, give_ref = refs
    total = keep_ref[...]
    for other_ref in other_refs:
        total = total + other_ref[...].astype(jnp.float32)
    next_keep_ref[...] = total[:1]
    give_ref[...] = total[1:].astype(jnp.bfloat16)


def mix_body(pick_ref, back_ref, out_ref):
    experts = back_ref.shape[0] // 2
    for m in range(pick_ref.shape[0]):
        part = slice(m * CAPS, (m + 1) * CAPS)
        halves = [
            back_ref.at[pl.ds(0, 2 * experts), part][...]
            .reshape(experts, 2, CAPS, -1)[:, h]
            .reshape(experts * CAPS, -1)
            for h in range(2)
        ]
        out_ref[m] = (
            dot(pick_ref[m], halves[0], (0, 0)) + dot(pick_ref[m], halves[1], (0, 0))
        ).astype(jnp.bfloat16)


def total_body(factor, keep_ref, other_ref, *out_refs):
    cols = out_refs[0].shape[1]
    total = (keep_ref[0] + other_ref[0].astype(jnp.float32)) * factor
    for k, out_ref in enumerate(out_refs):
        out_ref[...] = total[:, k * cols : (k + 1) * cols]


def per_device(grad_out, routes, route_probs, dispatched, w_gate, w_up, w_down):
    micro, tokens, width = grad_out.shape
    slots = dispatched.shape[1]
    cols = w_gate.shape[1]
    holders = lax.axis_size(EXPERT)
    pieces = lax.axis_size(DP)
    rows = width // pieces
    bf16, f32 = jnp.bfloat16, jnp.float32
    shape = jax.ShapeDtypeStruct

    send, pick = call(
        route_body,
        (
            shape((holders, micro * CAPS, width), bf16),
            shape((micro, holders // 2 * CAPS, tokens), bf16),
        ),
        1 << 27,
        [HBM] * 3,
        [
            pltpu.VMEM((micro, TOPK, tokens), jnp.int32),
            pltpu.VMEM((micro, TOPK, tokens), bf16),
            pltpu.VMEM(grad_out.shape, bf16),
            pltpu.VMEM((micro, holders, CAPS, width), bf16),
            pltpu.VMEM((micro, holders // 2 * CAPS, tokens), bf16),
            pltpu.SemaphoreType.DMA((3,)),
            pltpu.SemaphoreType.DMA((micro + 1,)),
        ],
        2,
        60,
    )(jnp.swapaxes(routes, 1, 2), jnp.swapaxes(route_probs, 1, 2), grad_out)
    got = lax.all_to_all(send, EXPERT, 0, 0, tiled=True)

    def lot(count):
        return count, rows, 3 * cols

    d_gate, d_up, keep, give = call(
        weight_body,
        (
            shape((micro * slots, cols), bf16),
            shape((micro * slots, cols), bf16),
            shape(lot(pieces // 2), f32),
            shape(lot(pieces // 2), bf16),
        ),
        1 << 31,
        [VMEM] * 5,
        [pltpu.VMEM((micro * slots, width), bf16), pltpu.VMEM(lot(pieces), f32)],
    )(got, dispatched, w_gate, w_up, w_down)
    (back_send,) = call(
        slot_body,
        (shape((holders, micro * CAPS, width), bf16),),
        1 << 30,
        [VMEM] * 4,
        [
            pltpu.VMEM((micro, holders, CAPS, width), bf16),
            pltpu.SemaphoreType.DMA((micro,)),
        ],
        1,
    )(d_gate, d_up, w_gate, w_up)
    back = lax.all_to_all(back_send, EXPERT, 0, 0, tiled=True)

    def swap(value, axis, partner):
        return lax.ppermute(
            value, axis, [(i, partner(i)) for i in range(lax.axis_size(axis))]
        )

    def small(body, count, sends, *values):
        return call(
            body,
            (shape(lot(count), f32), *[shape(lot(count), bf16)] * sends),
            1 << 20,
            [VMEM] * len(values),
        )(*values)

    other = swap(give, "core", near)
    keep, give = small(halve_body, pieces // 4, 1, keep, other)
    other = swap(give, "y", near)
    keep, *gives = small(spread_body, 2, len(TURNS), keep, other)
    others = [swap(give, "y", turn) for turn, give in zip(TURNS, gives)]
    keep, give = small(gather_body, 1, 1, keep, *others)
    other = swap(give, "zl", near)
    (grad_in,) = call(
        mix_body, (shape((micro, tokens, width), bf16),), 1 << 27, [VMEM] * 2
    )(pick, back)
    factor = 1.0 / (micro * pieces)
    grads = call(
        lambda *refs: total_body(factor, *refs),
        tuple(shape((rows, cols), f32) for _ in range(3)),
        1 << 20,
        [VMEM] * 2,
    )(keep, other)
    return (grad_in, *grads)


def solution(mesh):
    fine = Mesh(mesh.devices.reshape(2, 8, 2, 4, 2, 2), DP + EXPERT)
    tokens = P(None, ALL_DP, None)
    return jax.shard_map(
        per_device,
        mesh=fine,
        in_specs=(tokens, tokens, tokens, tokens, P(None, EXPERT), P(None, EXPERT), P(EXPERT, None)),
        out_specs=(tokens, P(DP, EXPERT), P(DP, EXPERT), P(DP, EXPERT)),
        check_vma=False,
    )
```

```python
import jax
import jax.numpy as jnp
from jax import lax
from jax.experimental import pallas as pl
from jax.experimental.pallas import tpu as pltpu
from jax.sharding import Mesh
from jax.sharding import PartitionSpec as P

TOPK = 8
CAPS = 8
DP = ("zl", "y", "core")
EXPERT = ("x", "zq", "zp")
ALL_DP = DP + EXPERT


def near(index):
    return index ^ 1


def plus(index):
    return (index + 2) & 7


def minus(index):
    return (index + 6) & 7


def cross(index):
    return (index + 5 - 2 * (index & 1)) & 7


TURNS = (cross, plus, minus)
PARTS = 4
VMEM = pl.BlockSpec(memory_space=pltpu.VMEM)
HBM = pl.BlockSpec(memory_space=pltpu.HBM)


def dot(left, right, contract):
    return lax.dot_general(
        left, right, ((contract[:1], contract[1:]), ((), ())), preferred_element_type=jnp.float32
    )


def call(body, outs, flops, specs, scratch=(), to_hbm=0, limit=20):
    return pl.pallas_call(
        body,
        out_shape=outs,
        in_specs=specs,
        out_specs=tuple(HBM if k < to_hbm else VMEM for k in range(len(outs))),
        scratch_shapes=list(scratch),
        compiler_params=pltpu.CompilerParams(vmem_limit_bytes=limit * 1024 * 1024),
        cost_estimate=pl.CostEstimate(flops=flops, bytes_accessed=4 << 20, transcendentals=0),
    )


def route_body(
    ids_hbm,
    probs_hbm,
    grad_hbm,
    send_hbm,
    pick_hbm,
    ids_ref,
    probs_ref,
    grad_ref,
    send_ref,
    pick_ref,
    sems,
    out_sems,
):
    copies = [
        pltpu.make_async_copy(source, goal, sems.at[k])
        for k, (source, goal) in enumerate(
            ((ids_hbm, ids_ref), (probs_hbm, probs_ref), (grad_hbm, grad_ref))
        )
    ]
    for copy in copies:
        copy.start()
    micro, _, tokens = ids_ref.shape
    holders, _, width = send_ref.shape[1:]
    rows = holders // 2 * CAPS
    row = lax.broadcasted_iota(jnp.int32, (rows, tokens), 0)
    expert = row // CAPS
    slot = (row % CAPS).astype(jnp.float32)
    earlier = (
        lax.broadcasted_iota(jnp.int32, (tokens, tokens), 0)
        < lax.broadcasted_iota(jnp.int32, (tokens, tokens), 1)
    ).astype(jnp.bfloat16)
    for copy in copies[:2]:
        copy.wait()
    weights = []
    for m in range(micro):
        weight = jnp.zeros((rows, tokens), jnp.float32)
        live = jnp.zeros((rows, tokens), jnp.float32)
        for k in range(TOPK):
            named = ids_ref[m, k : k + 1, :] == expert
            weight = jnp.where(named, probs_ref[m, k : k + 1, :].astype(jnp.float32), weight)
            live = jnp.where(named, 1.0, live)
        rank = dot(live.astype(jnp.bfloat16), earlier, (1, 0))
        chosen = jnp.logical_and(live > 0.0, rank == slot)
        pick_ref[m] = chosen.astype(jnp.bfloat16)
        weights.append(jnp.where(chosen, weight, 0.0).astype(jnp.bfloat16))
    copies[2].wait()
    puts = []
    for m in range(micro):
        scaled = dot(weights[m], grad_ref[m], (1, 0)).astype(jnp.bfloat16)
        send_ref[m] = jnp.broadcast_to(
            scaled.reshape(holders // 2, 1, CAPS, width), (holders // 2, 2, CAPS, width)
        ).reshape(holders, CAPS, width)
        puts.append(
            pltpu.make_async_copy(
                send_ref.at[m], send_hbm.at[:, pl.ds(m * CAPS, CAPS), :], out_sems.at[m]
            )
        )
        puts[-1].start()
    puts.append(pltpu.make_async_copy(pick_ref, pick_hbm, out_sems.at[micro]))
    puts[-1].start()
    for put in puts:
        put.wait()


def weight_body(
    got_ref,
    x_ref,
    gate_w_ref,
    up_w_ref,
    down_w_ref,
    d_both_ref,
    keep_ref,
    give_ref,
    got_all_ref,
    all_ref,
):
    micro, slots, width = x_ref.shape
    pieces, rows, _ = all_ref.shape
    cols = gate_w_ref.shape[1]
    x = x_ref[...].reshape(micro * slots, width)
    for m in range(micro):
        got_all_ref[m * slots : (m + 1) * slots] = got_ref[
            :, m * CAPS : (m + 1) * CAPS, :
        ].reshape(slots, width)
    gate = dot(x, gate_w_ref[...], (1, 0))
    up = dot(x, up_w_ref[...], (1, 0))
    sigmoid = jax.nn.sigmoid(gate)
    activated = gate * sigmoid
    hidden = (activated * up).astype(jnp.bfloat16)
    to_gate = up * sigmoid * (1.0 + gate * (1.0 - sigmoid))
    d_hidden = dot(got_all_ref[...], down_w_ref[...], (1, 1))
    d_both_ref[:, :cols] = (d_hidden * to_gate).astype(jnp.bfloat16)
    d_both_ref[:, cols:] = (d_hidden * activated).astype(jnp.bfloat16)
    total = dot(x, d_both_ref[...], (0, 0))
    all_ref[:, :, : 2 * cols] = total.reshape(pieces, rows, 2 * cols)
    total = dot(got_all_ref[...], hidden, (0, 0))
    all_ref[:, :, 2 * cols :] = total.reshape(pieces, rows, cols)
    plane, line, core = (lax.axis_index(axis) for axis in DP)
    for k in range(pieces // 2):
        goal = near(line) if k & 1 else line
        goal = TURNS[(k >> 2) - 1](goal) if k >> 2 else goal
        chip = ((plane ^ (k >> 1 & 1)) * lax.axis_size("y") + goal) * 2
        keep_ref[k] = all_ref[chip + core]
        give_ref[k] = all_ref[chip + near(core)].astype(jnp.bfloat16)


def slot_body(d_both_ref, gate_w_ref, up_w_ref, back_hbm, back_ref, sems):
    parts, micro, holders, _, width = back_ref.shape
    cols = gate_w_ref.shape[1]
    puts = []
    for n in range(parts):
        span = pl.ds(n * width, width)
        back = dot(d_both_ref[:, :cols], gate_w_ref[span, :], (1, 1)) + dot(
            d_both_ref[:, cols:], up_w_ref[span, :], (1, 1)
        )
        back_ref[n] = back.astype(jnp.bfloat16).reshape(micro, holders, CAPS, width)
        for m in range(micro):
            put = pltpu.make_async_copy(
                back_ref.at[n, m],
                back_hbm.at[:, pl.ds(m * CAPS, CAPS), span],
                sems.at[n * micro + m],
            )
            put.start()
            puts.append(put)
    for put in puts:
        put.wait()


def halve_body(keep_ref, other_ref, next_keep_ref, next_give_ref):
    for k in range(next_keep_ref.shape[0]):
        next_keep_ref[k] = keep_ref[2 * k] + other_ref[2 * k].astype(jnp.float32)
        next_give_ref[k] = (
            keep_ref[2 * k + 1] + other_ref[2 * k + 1].astype(jnp.float32)
        ).astype(jnp.bfloat16)


def spread_body(keep_ref, other_ref, next_keep_ref, *give_refs):
    for k in range(2):
        turns = [
            keep_ref[2 * t + k] + other_ref[2 * t + k].astype(jnp.float32)
            for t in range(1 + len(give_refs))
        ]
        next_keep_ref[k] = turns[0]
        for give_ref, turn in zip(give_refs, turns[1:]):
            give_ref[k] = turn.astype(jnp.bfloat16)


def gather_body(keep_ref, *refs):
    *other_refs, next_keep_ref, give_ref = refs
    total = keep_ref[...]
    for other_ref in other_refs:
        total = total + other_ref[...].astype(jnp.float32)
    next_keep_ref[...] = total[:1]
    give_ref[...] = total[1:].astype(jnp.bfloat16)


def mix_body(pick_ref, back_ref, out_ref):
    experts = back_ref.shape[0] // 2
    for m in range(pick_ref.shape[0]):
        part = slice(m * CAPS, (m + 1) * CAPS)
        halves = [
            back_ref.at[pl.ds(0, 2 * experts), part][...]
            .reshape(experts, 2, CAPS, -1)[:, h]
            .reshape(experts * CAPS, -1)
            for h in range(2)
        ]
        out_ref[m] = (
            dot(pick_ref[m], halves[0], (0, 0)) + dot(pick_ref[m], halves[1], (0, 0))
        ).astype(jnp.bfloat16)


def total_body(factor, keep_ref, other_ref, *out_refs):
    cols = out_refs[0].shape[1]
    total = (keep_ref[0] + other_ref[0].astype(jnp.float32)) * factor
    for k, out_ref in enumerate(out_refs):
        out_ref[...] = total[:, k * cols : (k + 1) * cols]


def per_device(grad_out, routes, route_probs, dispatched, w_gate, w_up, w_down):
    micro, tokens, width = grad_out.shape
    slots = dispatched.shape[1]
    cols = w_gate.shape[1]
    holders = lax.axis_size(EXPERT)
    pieces = lax.axis_size(DP)
    rows = width // pieces
    bf16, f32 = jnp.bfloat16, jnp.float32
    shape = jax.ShapeDtypeStruct

    send, pick = call(
        route_body,
        (
            shape((holders, micro * CAPS, width), bf16),
            shape((micro, holders // 2 * CAPS, tokens), bf16),
        ),
        1 << 27,
        [HBM] * 3,
        [
            pltpu.VMEM((micro, TOPK, tokens), jnp.int32),
            pltpu.VMEM((micro, TOPK, tokens), bf16),
            pltpu.VMEM(grad_out.shape, bf16),
            pltpu.VMEM((micro, holders, CAPS, width), bf16),
            pltpu.VMEM((micro, holders // 2 * CAPS, tokens), bf16),
            pltpu.SemaphoreType.DMA((3,)),
            pltpu.SemaphoreType.DMA((micro + 1,)),
        ],
        2,
        60,
    )(jnp.swapaxes(routes, 1, 2), jnp.swapaxes(route_probs, 1, 2), grad_out)
    got = lax.all_to_all(send, EXPERT, 0, 0, tiled=True)

    def lot(count):
        return count, rows, 3 * cols

    d_both, keep, give = call(
        weight_body,
        (
            shape((micro * slots, 2 * cols), bf16),
            shape(lot(pieces // 2), f32),
            shape(lot(pieces // 2), bf16),
        ),
        1 << 31,
        [VMEM] * 5,
        [pltpu.VMEM((micro * slots, width), bf16), pltpu.VMEM(lot(pieces), f32)],
    )(got, dispatched, w_gate, w_up, w_down)
    (back_send,) = call(
        slot_body,
        (shape((holders, micro * CAPS, width), bf16),),
        1 << 30,
        [VMEM] * 3,
        [
            pltpu.VMEM((PARTS, micro, holders, CAPS, width // PARTS), bf16),
            pltpu.SemaphoreType.DMA((PARTS * micro,)),
        ],
        1,
    )(d_both, w_gate, w_up)
    back = lax.all_to_all(back_send, EXPERT, 0, 0, tiled=True)

    def swap(value, axis, partner):
        return lax.ppermute(
            value, axis, [(i, partner(i)) for i in range(lax.axis_size(axis))]
        )

    def small(body, count, sends, *values):
        return call(
            body,
            (shape(lot(count), f32), *[shape(lot(count), bf16)] * sends),
            1 << 20,
            [VMEM] * len(values),
        )(*values)

    other = swap(give, "core", near)
    keep, give = small(halve_body, pieces // 4, 1, keep, other)
    other = swap(give, "y", near)
    keep, *gives = small(spread_body, 2, len(TURNS), keep, other)
    others = [swap(give, "y", turn) for turn, give in zip(TURNS, gives)]
    keep, give = small(gather_body, 1, 1, keep, *others)
    other = swap(give, "zl", near)
    (grad_in,) = call(
        mix_body, (shape((micro, tokens, width), bf16),), 1 << 27, [VMEM] * 2
    )(pick, back)
    factor = 1.0 / (micro * pieces)
    grads = call(
        lambda *refs: total_body(factor, *refs),
        tuple(shape((rows, cols), f32) for _ in range(3)),
        1 << 20,
        [VMEM] * 2,
    )(keep, other)
    return (grad_in, *grads)


def solution(mesh):
    fine = Mesh(mesh.devices.reshape(2, 8, 2, 4, 2, 2), DP + EXPERT)
    tokens = P(None, ALL_DP, None)
    return jax.shard_map(
        per_device,
        mesh=fine,
        in_specs=(tokens, tokens, tokens, tokens, P(None, EXPERT), P(None, EXPERT), P(EXPERT, None)),
        out_specs=(tokens, P(DP, EXPERT), P(DP, EXPERT), P(DP, EXPERT)),
        check_vma=False,
    )
```

```python
import jax
import jax.numpy as jnp
from jax import lax
from jax.experimental import pallas as pl
from jax.experimental.pallas import tpu as pltpu
from jax.sharding import Mesh
from jax.sharding import PartitionSpec as P

TOPK = 8
CAPS = 8
DP = ("zl", "y", "core")
EXPERT = ("x", "zq", "zp")
ALL_DP = DP + EXPERT


def near(index):
    return index ^ 1


def plus(index):
    return (index + 2) & 7


def minus(index):
    return (index + 6) & 7


def cross(index):
    return (index + 5 - 2 * (index & 1)) & 7


TURNS = (cross, plus, minus)
PARTS = 4
VMEM = pl.BlockSpec(memory_space=pltpu.VMEM)
HBM = pl.BlockSpec(memory_space=pltpu.HBM)


def dot(left, right, contract):
    return lax.dot_general(
        left, right, ((contract[:1], contract[1:]), ((), ())), preferred_element_type=jnp.float32
    )


def call(body, outs, flops, specs, scratch=(), to_hbm=0, limit=20):
    return pl.pallas_call(
        body,
        out_shape=outs,
        in_specs=specs,
        out_specs=tuple(HBM if k < to_hbm else VMEM for k in range(len(outs))),
        scratch_shapes=list(scratch),
        compiler_params=pltpu.CompilerParams(vmem_limit_bytes=limit * 1024 * 1024),
        cost_estimate=pl.CostEstimate(flops=flops, bytes_accessed=4 << 20, transcendentals=0),
    )


def route_body(
    ids_hbm,
    probs_hbm,
    grad_hbm,
    send_hbm,
    pick_hbm,
    ids_ref,
    probs_ref,
    grad_ref,
    send_ref,
    pick_ref,
    sems,
    out_sems,
):
    copies = [
        pltpu.make_async_copy(source, goal, sems.at[k])
        for k, (source, goal) in enumerate(
            ((ids_hbm, ids_ref), (probs_hbm, probs_ref), (grad_hbm, grad_ref))
        )
    ]
    for copy in copies:
        copy.start()
    micro, _, tokens = ids_ref.shape
    holders, _, width = send_ref.shape[1:]
    rows = holders // 2 * CAPS
    row = lax.broadcasted_iota(jnp.int32, (rows, tokens), 0)
    expert = row // CAPS
    slot = (row % CAPS).astype(jnp.float32)
    earlier = (
        lax.broadcasted_iota(jnp.int32, (tokens, tokens), 0)
        < lax.broadcasted_iota(jnp.int32, (tokens, tokens), 1)
    ).astype(jnp.bfloat16)
    for copy in copies[:2]:
        copy.wait()
    weights = []
    for m in range(micro):
        weight = jnp.zeros((rows, tokens), jnp.float32)
        live = jnp.zeros((rows, tokens), jnp.float32)
        for k in range(TOPK):
            named = ids_ref[m, k : k + 1, :] == expert
            weight = jnp.where(named, probs_ref[m, k : k + 1, :].astype(jnp.float32), weight)
            live = jnp.where(named, 1.0, live)
        rank = dot(live.astype(jnp.bfloat16), earlier, (1, 0))
        chosen = jnp.logical_and(live > 0.0, rank == slot)
        pick_ref[m] = chosen.astype(jnp.bfloat16)
        weights.append(jnp.where(chosen, weight, 0.0).astype(jnp.bfloat16))
    copies[2].wait()
    puts = []
    for m in range(micro):
        scaled = dot(weights[m], grad_ref[m], (1, 0)).astype(jnp.bfloat16)
        send_ref[m] = jnp.broadcast_to(
            scaled.reshape(holders // 2, 1, CAPS, width), (holders // 2, 2, CAPS, width)
        ).reshape(holders, CAPS, width)
        puts.append(
            pltpu.make_async_copy(
                send_ref.at[m], send_hbm.at[:, pl.ds(m * CAPS, CAPS), :], out_sems.at[m]
            )
        )
        puts[-1].start()
    puts.append(pltpu.make_async_copy(pick_ref, pick_hbm, out_sems.at[micro]))
    puts[-1].start()
    for put in puts:
        put.wait()


def weight_body(
    got_ref,
    x_ref,
    gate_w_ref,
    up_w_ref,
    down_w_ref,
    d_both_ref,
    keep_ref,
    give_ref,
    got_all_ref,
    all_ref,
):
    micro, slots, width = x_ref.shape
    pieces, rows, _ = all_ref.shape
    cols = gate_w_ref.shape[1]
    x = x_ref[...].reshape(micro * slots, width)
    for m in range(micro):
        got_all_ref[m * slots : (m + 1) * slots] = got_ref[
            :, m * CAPS : (m + 1) * CAPS, :
        ].reshape(slots, width)
    hidden = []
    half = micro * slots // 2
    for start in (0, half):
        span = slice(start, start + half)
        gate = dot(x[span], gate_w_ref[...], (1, 0))
        up = dot(x[span], up_w_ref[...], (1, 0))
        d_hidden = dot(got_all_ref[span], down_w_ref[...], (1, 1))
        sigmoid = jax.nn.sigmoid(gate)
        activated = gate * sigmoid
        hidden.append((activated * up).astype(jnp.bfloat16))
        to_gate = up * sigmoid * (1.0 + gate * (1.0 - sigmoid))
        d_both_ref[span, :cols] = (d_hidden * to_gate).astype(jnp.bfloat16)
        d_both_ref[span, cols:] = (d_hidden * activated).astype(jnp.bfloat16)
    hidden = jnp.concatenate(hidden, axis=0)
    total = dot(x, d_both_ref[...], (0, 0))
    all_ref[:, :, : 2 * cols] = total.reshape(pieces, rows, 2 * cols)
    total = dot(got_all_ref[...], hidden, (0, 0))
    all_ref[:, :, 2 * cols :] = total.reshape(pieces, rows, cols)
    plane, line, core = (lax.axis_index(axis) for axis in DP)
    for k in range(pieces // 2):
        goal = near(line) if k & 1 else line
        goal = TURNS[(k >> 2) - 1](goal) if k >> 2 else goal
        chip = ((plane ^ (k >> 1 & 1)) * lax.axis_size("y") + goal) * 2
        keep_ref[k] = all_ref[chip + core]
        give_ref[k] = all_ref[chip + near(core)].astype(jnp.bfloat16)


def slot_body(d_both_ref, gate_w_ref, up_w_ref, back_hbm, back_ref, sems):
    parts, micro, holders, _, width = back_ref.shape
    cols = gate_w_ref.shape[1]
    puts = []
    for n in range(parts):
        span = pl.ds(n * width, width)
        back = dot(d_both_ref[:, :cols], gate_w_ref[span, :], (1, 1)) + dot(
            d_both_ref[:, cols:], up_w_ref[span, :], (1, 1)
        )
        back_ref[n] = back.astype(jnp.bfloat16).reshape(micro, holders, CAPS, width)
        for m in range(micro):
            put = pltpu.make_async_copy(
                back_ref.at[n, m],
                back_hbm.at[:, pl.ds(m * CAPS, CAPS), span],
                sems.at[n * micro + m],
            )
            put.start()
            puts.append(put)
    for put in puts:
        put.wait()


def halve_body(keep_ref, other_ref, next_keep_ref, next_give_ref):
    for k in range(next_keep_ref.shape[0]):
        next_keep_ref[k] = keep_ref[2 * k] + other_ref[2 * k].astype(jnp.float32)
        next_give_ref[k] = (
            keep_ref[2 * k + 1] + other_ref[2 * k + 1].astype(jnp.float32)
        ).astype(jnp.bfloat16)


def spread_body(keep_ref, other_ref, next_keep_ref, *give_refs):
    for k in range(2):
        turns = [
            keep_ref[2 * t + k] + other_ref[2 * t + k].astype(jnp.float32)
            for t in range(1 + len(give_refs))
        ]
        next_keep_ref[k] = turns[0]
        for give_ref, turn in zip(give_refs, turns[1:]):
            give_ref[k] = turn.astype(jnp.bfloat16)


def gather_body(keep_ref, *refs):
    *other_refs, next_keep_ref, give_ref = refs
    total = keep_ref[...]
    for other_ref in other_refs:
        total = total + other_ref[...].astype(jnp.float32)
    next_keep_ref[...] = total[:1]
    give_ref[...] = total[1:].astype(jnp.bfloat16)


def mix_body(pick_ref, back_ref, out_ref):
    experts = back_ref.shape[0] // 2
    for m in range(pick_ref.shape[0]):
        part = slice(m * CAPS, (m + 1) * CAPS)
        halves = [
            back_ref.at[pl.ds(0, 2 * experts), part][...]
            .reshape(experts, 2, CAPS, -1)[:, h]
            .reshape(experts * CAPS, -1)
            for h in range(2)
        ]
        out_ref[m] = (
            dot(pick_ref[m], halves[0], (0, 0)) + dot(pick_ref[m], halves[1], (0, 0))
        ).astype(jnp.bfloat16)


def total_body(factor, keep_ref, other_ref, *out_refs):
    cols = out_refs[0].shape[1]
    total = (keep_ref[0] + other_ref[0].astype(jnp.float32)) * factor
    for k, out_ref in enumerate(out_refs):
        out_ref[...] = total[:, k * cols : (k + 1) * cols]


def per_device(grad_out, routes, route_probs, dispatched, w_gate, w_up, w_down):
    micro, tokens, width = grad_out.shape
    slots = dispatched.shape[1]
    cols = w_gate.shape[1]
    holders = lax.axis_size(EXPERT)
    pieces = lax.axis_size(DP)
    rows = width // pieces
    bf16, f32 = jnp.bfloat16, jnp.float32
    shape = jax.ShapeDtypeStruct

    send, pick = call(
        route_body,
        (
            shape((holders, micro * CAPS, width), bf16),
            shape((micro, holders // 2 * CAPS, tokens), bf16),
        ),
        1 << 27,
        [HBM] * 3,
        [
            pltpu.VMEM((micro, TOPK, tokens), jnp.int32),
            pltpu.VMEM((micro, TOPK, tokens), bf16),
            pltpu.VMEM(grad_out.shape, bf16),
            pltpu.VMEM((micro, holders, CAPS, width), bf16),
            pltpu.VMEM((micro, holders // 2 * CAPS, tokens), bf16),
            pltpu.SemaphoreType.DMA((3,)),
            pltpu.SemaphoreType.DMA((micro + 1,)),
        ],
        2,
        60,
    )(jnp.swapaxes(routes, 1, 2), jnp.swapaxes(route_probs, 1, 2), grad_out)
    got = lax.all_to_all(send, EXPERT, 0, 0, tiled=True)

    def lot(count):
        return count, rows, 3 * cols

    d_both, keep, give = call(
        weight_body,
        (
            shape((micro * slots, 2 * cols), bf16),
            shape(lot(pieces // 2), f32),
            shape(lot(pieces // 2), bf16),
        ),
        1 << 31,
        [VMEM] * 5,
        [pltpu.VMEM((micro * slots, width), bf16), pltpu.VMEM(lot(pieces), f32)],
    )(got, dispatched, w_gate, w_up, w_down)
    (back_send,) = call(
        slot_body,
        (shape((holders, micro * CAPS, width), bf16),),
        1 << 30,
        [VMEM] * 3,
        [
            pltpu.VMEM((PARTS, micro, holders, CAPS, width // PARTS), bf16),
            pltpu.SemaphoreType.DMA((PARTS * micro,)),
        ],
        1,
    )(d_both, w_gate, w_up)
    back = lax.all_to_all(back_send, EXPERT, 0, 0, tiled=True)

    def swap(value, axis, partner):
        return lax.ppermute(
            value, axis, [(i, partner(i)) for i in range(lax.axis_size(axis))]
        )

    def small(body, count, sends, *values):
        return call(
            body,
            (shape(lot(count), f32), *[shape(lot(count), bf16)] * sends),
            1 << 20,
            [VMEM] * len(values),
        )(*values)

    other = swap(give, "core", near)
    keep, give = small(halve_body, pieces // 4, 1, keep, other)
    other = swap(give, "y", near)
    keep, *gives = small(spread_body, 2, len(TURNS), keep, other)
    others = [swap(give, "y", turn) for turn, give in zip(TURNS, gives)]
    keep, give = small(gather_body, 1, 1, keep, *others)
    other = swap(give, "zl", near)
    (grad_in,) = call(
        mix_body, (shape((micro, tokens, width), bf16),), 1 << 27, [VMEM] * 2
    )(pick, back)
    factor = 1.0 / (micro * pieces)
    grads = call(
        lambda *refs: total_body(factor, *refs),
        tuple(shape((rows, cols), f32) for _ in range(3)),
        1 << 20,
        [VMEM] * 2,
    )(keep, other)
    return (grad_in, *grads)


def solution(mesh):
    fine = Mesh(mesh.devices.reshape(2, 8, 2, 4, 2, 2), DP + EXPERT)
    tokens = P(None, ALL_DP, None)
    return jax.shard_map(
        per_device,
        mesh=fine,
        in_specs=(tokens, tokens, tokens, tokens, P(None, EXPERT), P(None, EXPERT), P(EXPERT, None)),
        out_specs=(tokens, P(DP, EXPERT), P(DP, EXPERT), P(DP, EXPERT)),
        check_vma=False,
    )
```
